256 devices in a mesh: seq: 64 (over x, z, core), grp: 4 (over y).
Axes of the slice: x: 4, y: 4, z: 8, core: 2. Of those that a mesh axis runs over, the one named last changes fastest.
Arguments:
- delta_codes: int32 [16, 16, 16384, 128], P('grp', None, 'seq'), may hold values from -63 to 63, as said below
- scale_index: int32 [16, 16, 1024], P('grp', None, 'seq'), may hold values from 0 to 15
- anchor_codes: int32 [16, 16, 128], P('grp'), may hold values from -8 to 7
- scale_table: float32 [16, 128], replicated, may hold values from 5e-05 to 0.0005
- anchor_scale: float32 [128], replicated, may hold values from 0.0001 to 0.001
Outputs:
- decode_cache: bfloat16 [4, 64, 16384, 128], P('grp', 'seq')
The draws below stay inside these ranges and needn't reach their ends.
Inputs may be any that keep to these rules, and one draw needn't show every extreme that they name: `delta_codes`: for every sequence, head and channel, the running sum of the codes from the sequence's first token lies in -32 .. 31 after every token, and in -2 .. 1 after the last token of each group of 16 tokens.
All inputs are finite; a program needn't handle non-finite values.
Results may differ from the reference program's by a relative error of at most 0.001.
Values may be sent and summed in bfloat16 or wider, within the bound.
No kernel may reach another device: no remote copies, remote signals or barrier semaphores. Data moves between devices by JAX's collectives and lax.ppermute only.
A program may use at most 128 MiB of HBM per device.

```python
import math
import jax
import jax.numpy as jnp
from jax import lax

HEAD_DIM = 128
KV_HEADS = 16
GROUP_LEN = 16
LEVELS = 16
SEQS = 16
LENGTH = 16384
N_GRP = 4


def draw_delta_codes(key, part):
    running_key = jax.random.fold_in(key, 11)
    running = jax.random.randint(running_key, (SEQS, KV_HEADS, LENGTH, HEAD_DIM), -32, 32, dtype=jnp.int32)
    position = lax.broadcasted_iota(jnp.int32, (1, 1, LENGTH, 1), 2)
    group_end = position % GROUP_LEN == GROUP_LEN - 1
    running = jnp.where(group_end, jnp.remainder(running, 4) - 2, running)
    earlier = jnp.pad(running[:, :, :-1, :], ((0, 0), (0, 0), (1, 0), (0, 0)))
    return running - earlier


def plant(values, key, low, largest):
    dims = values.shape
    place = [jax.random.randint(jax.random.fold_in(key, axis), (), 0, dims[axis]) for axis in range(len(dims))]
    values = values.at[tuple(place)].set(low)
    longest = dims.index(max(dims))
    place[longest] = (place[longest] + 1) % dims[longest]
    return values.at[tuple(place)].set(largest)


def setup_inputs(seed: int = 0) -> dict:
    seeds = jax.random.split(jax.random.key(seed), 6)
    delta_codes = draw_delta_codes(jax.random.fold_in(seeds[5], 71), 0)
    scale_index = plant(jax.random.randint(seeds[1], (SEQS, KV_HEADS, LENGTH // GROUP_LEN), 0, LEVELS), jax.random.fold_in(seeds[1], 1), 0, LEVELS - 1).astype(jnp.int32)
    anchor_codes = plant(jax.random.randint(seeds[2], (SEQS, KV_HEADS, HEAD_DIM), -8, 8), jax.random.fold_in(seeds[2], 1), -8, 7).astype(jnp.int32)
    scale_table = jnp.clip(jnp.exp(jax.random.uniform(seeds[3], (LEVELS, HEAD_DIM), jnp.float32, math.log(4.999999873689376e-05), math.log(0.0005))), 4.999999873689376e-05, 0.0005)
    anchor_scale = jnp.clip(jnp.exp(jax.random.uniform(seeds[4], (HEAD_DIM,), jnp.float32, math.log(0.0001), math.log(0.001))), 0.0001, 0.001)
    return {"delta_codes": delta_codes, "scale_index": scale_index, "anchor_codes": anchor_codes, "scale_table": scale_table, "anchor_scale": anchor_scale}


def reference(delta_codes, scale_index, anchor_codes, scale_table, anchor_scale):
    def one_sequence(items):
        code_vals, scale_ids, anchors = items
        scales = scale_table[scale_ids]
        shaped = code_vals.astype(jnp.float32).reshape(KV_HEADS, LENGTH // GROUP_LEN, GROUP_LEN, HEAD_DIM)
        deltas = shaped * scales[:, :, None, :]
        summed = jnp.cumsum(deltas.reshape(KV_HEADS, LENGTH, HEAD_DIM), axis=1)
        anchor_vals = anchors.astype(jnp.float32) * anchor_scale
        return (summed + anchor_vals[:, None, :]).astype(jnp.bfloat16)

    rebuilt = lax.map(one_sequence, (delta_codes, scale_index, anchor_codes))
    arranged = rebuilt.reshape(SEQS, N_GRP, KV_HEADS // N_GRP, LENGTH, HEAD_DIM).transpose(1, 0, 2, 3, 4)
    return arranged.reshape(N_GRP, SEQS * (KV_HEADS // N_GRP), LENGTH, HEAD_DIM)
```

```python
import functools

import jax
import jax.numpy as jnp
from jax import lax
from jax.experimental import pallas as pl
from jax.experimental.pallas import tpu as pltpu
from jax.sharding import PartitionSpec as P

AXES = ("seq", "grp")
NX, NY, NZ, NC = 4, 4, 8, 2
HALF = 128
EXTRA = 8


def device(x, y, z, c):
    return (x * NZ * NC + z * NC + c) * NY + y


def every():
    return [(x, y, z, c) for x in range(NX) for y in range(NY) for z in range(NZ) for c in range(NC)]


ZC_GROUPS = [
    [device(x, y, z, c) for z in range(NZ) for c in range(NC)] for x in range(NX) for y in range(NY)
]


def y_pairs(r):
    return [(device(x, y, z, c), device(x, (y + x + r) % 4, z, c)) for x, y, z, c in every()]


def x_pairs(r):
    return [(device(x, y, z, c), device((y - x - r) % 4, y, z, c)) for x, y, z, c in every()]


def zc_all_to_all(v):
    return lax.all_to_all(
        v, AXES, split_axis=0, concat_axis=0, tiled=True, axis_index_groups=ZC_GROUPS
    )


def head_of(r):
    x = lax.axis_index("seq") // (NZ * NC)
    y = lax.axis_index("grp")
    return lax.rem(x + y + r, 4)


def group_sums(codes, lower):
    return jnp.dot(
        lower, codes.astype(jnp.float32).astype(jnp.bfloat16), preferred_element_type=jnp.float32
    ).astype(jnp.bfloat16)


def lower_blocks():
    row = lax.broadcasted_iota(jnp.int32, (HALF, HALF), 0)
    col = lax.broadcasted_iota(jnp.int32, (HALF, HALF), 1)
    return ((row // 16 == col // 16) & (row >= col)).astype(jnp.float32).astype(jnp.bfloat16)


def send_b_kernel(codes, ids, anchors, out):
    lower = lower_blocks()
    row = lax.broadcasted_iota(jnp.int32, (EXTRA, 128), 0)
    for r in range(4):
        h = head_of(r)
        id_tile = ids[0, h].astype(jnp.float32)
        id_tile = jnp.concatenate([id_tile, jnp.zeros((4, 112), jnp.float32)], axis=1)
        anchor_tile = anchors[0, h].astype(jnp.float32)
        for q in range(4):
            out[0, q, r, 0:HALF, :] = group_sums(codes[0, h, q], lower)
            tile = jnp.where(row == 0, id_tile[q : q + 1], jnp.where(row == 1, anchor_tile[q : q + 1], 0.0))
            out[0, q, r, HALF : HALF + EXTRA, :] = tile.astype(jnp.bfloat16)


def send_b(codes, ids, anchors):
    return pl.pallas_call(
        send_b_kernel,
        grid=(4,),
        in_specs=[
            pl.BlockSpec((1, 4, 4, HALF, 128), lambda b: (b, 0, 0, 1, 0)),
            pl.BlockSpec((1, 4, 4, 16), lambda b: (b, 0, 0, 0)),
            pl.BlockSpec((1, 4, 4, 128), lambda b: (b, 0, 0, 0)),
        ],
        out_specs=pl.BlockSpec((1, 4, 4, HALF + EXTRA, 128), lambda b: (b, 0, 0, 0, 0)),
        out_shape=jax.ShapeDtypeStruct((4, 4, 4, HALF + EXTRA, 128), jnp.bfloat16),
        cost_estimate=pl.CostEstimate(flops=4_000_000_000, bytes_accessed=6_000_000, transcendentals=0),
        name="send_b",
    )(codes, ids, anchors)


def send_a_kernel(codes, *outs):
    lower = lower_blocks()
    for r in range(4):
        h = head_of(r)
        for q in range(4):
            outs[r][0, q] = group_sums(codes[0, h, q], lower)


def send_a(codes, sub):
    return pl.pallas_call(
        send_a_kernel,
        grid=(2,),
        in_specs=[pl.BlockSpec((1, 4, 4, HALF, 128), lambda b: (b + 2 * sub, 0, 0, 0, 0))],
        out_specs=[pl.BlockSpec((1, 4, HALF, 128), lambda b: (b, 0, 0, 0))] * 4,
        out_shape=[jax.ShapeDtypeStruct((2, 4, HALF, 128), jnp.bfloat16)] * 4,
        cost_estimate=pl.CostEstimate(flops=2_000_000_000, bytes_accessed=3_000_000, transcendentals=0),
        name="send_a",
    )(codes)


def source_round(x_src):
    x = lax.axis_index("seq") // (NZ * NC)
    y = lax.axis_index("grp")
    return lax.rem(y - x - x_src + 8, 4)


def last_rows():
    row = lax.broadcasted_iota(jnp.int32, (8, HALF), 0)
    col = lax.broadcasted_iota(jnp.int32, (8, HALF), 1)
    return (col == row * 16 + 15).astype(jnp.float32).astype(jnp.bfloat16)


def scales_kernel(b, table, anchor_scale, scales, totals, anchor):
    pick = last_rows()
    level = lax.broadcasted_iota(jnp.int32, (16, 16), 0).astype(jnp.float32)

    def block(s, carry):
        rnd = source_round(s // 16)
        zc = lax.rem(s, 16)
        tile = b[rnd, zc, HALF : HALF + EXTRA, :].astype(jnp.float32)
        onehot = (jnp.broadcast_to(tile[0:1, 0:16], (16, 16)) == level).astype(jnp.float32)
        found = lax.dot_general(
            onehot,
            table[...],
            (((0,), (0,)), ((), ())),
            precision=lax.Precision.HIGHEST,
            preferred_element_type=jnp.float32,
        )
        scales[s] = found
        sums = jnp.dot(pick, b[rnd, zc, 0:HALF, :], preferred_element_type=jnp.float32)
        totals[s] = sums * found[8:16]
        return carry

    lax.fori_loop(0, 64, block, 0, unroll=4)
    first = b[source_round(0), 0, HALF : HALF + EXTRA, :].astype(jnp.float32)
    anchor[...] = first[1:2] * anchor_scale[...]


def make_scales(b, table, anchor_scale):
    return pl.pallas_call(
        scales_kernel,
        out_shape=[
            jax.ShapeDtypeStruct((64, 16, 128), jnp.float32),
            jax.ShapeDtypeStruct((64, 8, 128), jnp.float32),
            jax.ShapeDtypeStruct((1, 128), jnp.float32),
        ],
        cost_estimate=pl.CostEstimate(flops=4_000_000_000, bytes_accessed=3_000_000, transcendentals=0),
        name="make_scales",
    )(b, table, anchor_scale)


def rebuild_kernel(a, b, scales, totals, anchor, out, base):
    step = pl.program_id(0)

    @pl.when(step == 0)
    def _():
        pick = last_rows()
        row = lax.broadcasted_iota(jnp.int32, (HALF, HALF), 0)
        col = lax.broadcasted_iota(jnp.int32, (HALF, HALF), 1)
        strict = (row > col).astype(jnp.float32)
        carry = anchor[...]
        for i in range(8):
            parts = []
            for s in range(8 * i, 8 * i + 8):
                rnd = source_round(s // 16)
                sums = jnp.dot(pick, a[s % 16, rnd], preferred_element_type=jnp.float32)
                parts += [sums * scales[s, 0:8], totals[s]]
            steps = jnp.concatenate(parts, axis=0)
            before = (
                jnp.dot(strict, steps, precision=lax.Precision.HIGHEST, preferred_element_type=jnp.float32)
                + carry
            )
            carry = before[HALF - 1 :] + steps[HALF - 1 :]
            base[8 * i : 8 * i + 8] = before.reshape(8, 16, 128)

    for i in range(4):
        s = step * 4 + i
        rnd = source_round(s // 16)
        zc = lax.rem(s, 16)
        for part in range(2):
            codes = a[zc, rnd] if part == 0 else b[rnd, zc, 0:HALF, :]
            codes = codes.astype(jnp.float32).reshape(8, 16, 128)
            scale = scales[s, 8 * part : 8 * part + 8]
            start = base[s, 8 * part : 8 * part + 8]
            values = codes * scale[:, None, :] + start[:, None, :]
            at = i * 256 + part * HALF
            out[0, 0, at : at + HALF, :] = values.reshape(HALF, 128).astype(jnp.bfloat16)


def rebuild(a, b, scales, totals, anchor):
    whole = lambda *shape: pl.BlockSpec(shape, lambda i: (0,) * len(shape))
    return pl.pallas_call(
        rebuild_kernel,
        grid=(16,),
        in_specs=[
            whole(16, 4, HALF, 128),
            whole(4, 16, HALF + EXTRA, 128),
            whole(64, 16, 128),
            whole(64, 8, 128),
            whole(1, 128),
        ],
        out_specs=pl.BlockSpec((1, 1, 1024, 128), lambda i: (0, 0, i, 0)),
        out_shape=jax.ShapeDtypeStruct((1, 1, 16384, 128), jnp.bfloat16),
        scratch_shapes=[pltpu.VMEM((64, 16, 128), jnp.float32)],
        name="rebuild",
    )(a, b, scales, totals, anchor)


def on_device(delta_codes, scale_index, anchor_codes, scale_table, anchor_scale):
    codes = delta_codes.reshape(4, 4, 4, 256, 128)
    b = send_b(codes, scale_index.reshape(4, 4, 4, 16), anchor_codes.reshape(4, 4, 4, 128))
    b = zc_all_to_all(b.reshape(16, 4, HALF + EXTRA, 128))
    a_parts = []
    for sub in range(2):
        sent = send_a(codes, sub)
        rows = []
        for r in range(4):
            v = lax.ppermute(sent[r].reshape(8, HALF, 128), AXES, y_pairs(r))
            v = lax.ppermute(v, AXES, x_pairs(r))
            rows.append(v)
        a_parts.append(jnp.stack(rows, axis=1))
    a = zc_all_to_all(jnp.concatenate(a_parts, axis=0))
    b_rounds = []
    for r in range(4):
        halves = []
        for sub in range(2):
            v = b[8 * sub : 8 * sub + 8, r]
            v = lax.ppermute(v, AXES, y_pairs(r))
            v = lax.ppermute(v, AXES, x_pairs(r))
            halves.append(v)
        b_rounds.append(jnp.concatenate(halves, axis=0))
    b = jnp.stack(b_rounds)
    scales, totals, anchor = make_scales(b, scale_table, anchor_scale.reshape(1, 128))
    return rebuild(a, b, scales, totals, anchor)


def solution(mesh):
    placed = (P("grp", None, "seq", None), P("grp", None, "seq"), P("grp", None, None), P(), P())
    return jax.shard_map(
        on_device,
        mesh=mesh,
        in_specs=placed,
        out_specs=P("grp", "seq", None, None),
        check_vma=False,
    )
```
